32 devices in a mesh: member: 8 (over z, y), region: 4 (over x, core).
Axes of the slice: x: 2, y: 2, z: 4, core: 2. Of those that a mesh axis runs over, the one named last changes fastest.
Arguments:
- ensemble: bfloat16 [512, 32768], P(('member', 'region')), may hold values from -12 to 12
- obs_offset: int32 [4, 8, 16], P('region', 'member'), may hold values from 0 to 1023
- observed: float32 [4, 8, 16], P('region', 'member'), may hold values from -12 to 12
- obs_var: float32 [4, 8, 16], P('region', 'member'), may hold values from 0.2 to 2
Outputs:
- analysis: bfloat16 [512, 32768], P(('member', 'region'))
The draws below stay inside these ranges and needn't reach their ends.
Inputs may be any that keep to these rules, and one draw needn't show every extreme that they name: obs_offset indexes a link within the block of 1024 links; two detectors may watch the same link.
All inputs are finite; a program needn't handle non-finite values.
Results may differ from the reference program's by a relative error of at most 0.0019.
Values may be sent and summed in bfloat16 or wider, within the bound.
A program may use at most 128 MiB of HBM per device.

```python
import math
import jax
import jax.numpy as jnp
from jax import lax

M = 512
LINK_DEV = 1024
OBS_DEV = 16
REGION_LINKS = 8192
S = 32768
N_MEMBER = 8
N_REGION = 4


def draw_ensemble(key, part):
    values = jax.random.normal(key, (M, S), jnp.float32)
    return jnp.clip(values, -6.0, 6.0).astype(jnp.bfloat16)


def place_ends(entries, stream_key, smallest, top_value):
    place = [jax.random.randint(jax.random.fold_in(stream_key, axis), (), 0, length) for axis, length in enumerate(entries.shape)]
    widest = entries.shape.index(max(entries.shape))
    beside = place[:widest] + [(place[widest] + 1) % entries.shape[widest]] + place[widest + 1:]
    return entries.at[tuple(place)].set(smallest).at[tuple(beside)].set(top_value)


def block_levels(key, shape, shards, low, high):
    loudness = 1.0
    for axis_at, parts in shards:
        steps = jax.random.uniform(jax.random.fold_in(jax.random.fold_in(key, 6), axis_at), (parts,), jnp.float32, low / len(shards), high / len(shards))
        loudness = loudness * jnp.repeat(jnp.exp(steps), shape[axis_at] // parts).reshape((-1,) + (1,) * (len(shape) - 1 - axis_at))
    return loudness


def scatter_about(rng, shape, scale, bound, pieces=(), kind=jnp.bfloat16):
    level = block_levels(rng, shape, pieces, -0.22, 0.18) if pieces else 1.0
    entries = jax.random.normal(rng, shape, jnp.float32) * scale * level
    return jnp.minimum(jnp.maximum(entries, -bound), bound).astype(kind)


def setup_inputs(seed: int = 0) -> dict:
    streams_of = jax.random.split(jax.random.key(seed), 5)
    return {
        "ensemble": draw_ensemble(jax.random.fold_in(streams_of[4], 71), 0),
        "obs_offset": place_ends(jax.random.randint(streams_of[1], (N_REGION, N_MEMBER, OBS_DEV), 0, LINK_DEV), jax.random.fold_in(streams_of[1], 1), 0, LINK_DEV - 1).astype(jnp.int32),
        "observed": scatter_about(streams_of[2], (N_REGION, N_MEMBER, OBS_DEV), 2.0, 12.0, ((0, 4), (1, 8)), jnp.float32),
        "obs_var": jnp.clip(jnp.exp(math.log(2.0) - 2.3025851 * jax.random.uniform(streams_of[3], (N_REGION, N_MEMBER, OBS_DEV), jnp.float32) ** block_levels(streams_of[3], (N_REGION, N_MEMBER, OBS_DEV), ((0, 4), (1, 8)), -0.2, 0.2)), 0.2, 2.0),
    }


def observation_terms(picked, values, variance, ensemble_size):
    center = lax.optimization_barrier(jnp.mean(picked, axis=1, keepdims=True))
    anomaly = picked - center
    innovation = values - center[:, 0]
    numer = jnp.sum(innovation * innovation)
    denom = jnp.sum(lax.optimization_barrier(jnp.sum(anomaly * anomaly, axis=1)) / (ensemble_size - 1.0) + variance)
    weight = 1.0 / ((ensemble_size - 1.0) * variance)
    return (anomaly, innovation, weight, numer, denom)

def weighted_products(anomaly, innovation, weight):
    weighted = anomaly * weight[:, None]
    products = jnp.dot(weighted.T, anomaly, precision=lax.Precision.HIGHEST)
    column = jnp.dot(innovation * weight, anomaly, precision=lax.Precision.HIGHEST)
    return (products, column)

def mixing_matrix(products, column, lift, diag_coef, col_coef, mat_coef):
    identity = jnp.eye(products.shape[0], dtype=jnp.float32)
    system = identity + lift * products
    factor = jnp.linalg.cholesky(system)
    right_side = jnp.concatenate([products, column[:, None]], axis=1)
    solved = jax.scipy.linalg.cho_solve((factor, True), right_side)
    return diag_coef * identity + col_coef * solved[:, -1][None, :] - mat_coef * solved[:, :-1]

def reference(ensemble, obs_offset, observed, obs_var):
    ensemble_size = ensemble.shape[0]
    link_total = ensemble.shape[1]
    region_idx = lax.broadcasted_iota(jnp.int32, obs_offset.shape, 0)
    member_idx = lax.broadcasted_iota(jnp.int32, obs_offset.shape, 1)
    link_index = (region_idx * REGION_LINKS + member_idx * LINK_DEV + obs_offset.astype(jnp.int32)).reshape(-1).astype(jnp.int32)
    picked = jnp.take(ensemble, link_index, axis=1).T.astype(jnp.float32)
    anomaly, innovation, weight, numer, denom = observation_terms(picked, observed.reshape(-1), obs_var.reshape(-1), ensemble_size)
    products, column = weighted_products(anomaly, innovation, weight)
    inflation = jnp.sqrt(numer / denom)
    mixing = mixing_matrix(products, column, inflation * inflation, inflation, inflation * inflation, 0.5 * inflation * inflation * inflation)

    def update_block(block):
        state_values = block.astype(jnp.float32)
        center = lax.optimization_barrier(jnp.mean(state_values, axis=0, keepdims=True))
        return (center + jnp.dot(mixing, state_values - center, precision=lax.Precision.HIGHEST)).astype(jnp.bfloat16)
    blocks = jnp.moveaxis(ensemble.reshape(ensemble_size, -1, LINK_DEV), 1, 0)
    updated = lax.map(update_block, blocks)
    return jnp.moveaxis(updated, 0, 1).reshape(ensemble_size, link_total)
```

```python
import functools

import jax
import jax.numpy as jnp
from jax import lax
from jax.experimental import pallas as pl
from jax.experimental.pallas import tpu as pltpu
from jax.sharding import PartitionSpec as P

MESH = pl.DeviceIdType.MESH
F32 = jnp.float32
BF16 = jnp.bfloat16
VMEM_LIMIT = 48 * 1024 * 1024


def peers(members, regions):
    count = members * regions
    own_member, own_region = lax.axis_index("member"), lax.axis_index("region")
    me = own_member * regions + own_region

    def peer(step):
        other = (me + step) % count
        return other, other // regions, other % regions

    return count, me, own_region * members + own_member, peer


def entry_barrier(count, peer):
    barrier = pltpu.get_barrier_semaphore()

    def greet(step, carry):
        _, m, g = peer(step)
        pl.semaphore_signal(barrier, inc=1, device_id=(m, g), device_id_type=MESH)
        return carry

    lax.fori_loop(1, count, greet, 0)
    pl.semaphore_wait(barrier, count - 1)


def gather_kernel(members, regions, ens, off, aux, x_out, picks_out, aux_out, off_all, own_picks,
                  off_send, off_recv, aux_send, aux_recv, x_send, x_recv, pick_send, pick_recv, local_sem):
    count, me, my_block, peer = peers(members, regions)
    links = x_out.shape[2]
    obs = off.shape[0]

    own_off = pltpu.make_async_copy(off, off_all.at[my_block], local_sem.at[0])
    own_aux = pltpu.make_async_copy(aux, aux_out.at[my_block], local_sem.at[1])
    own_x = pltpu.make_async_copy(
        ens.at[:, pl.ds(pl.multiple_of(my_block * links, links), links)], x_out.at[me], local_sem.at[2])
    own_off.start()
    own_aux.start()
    own_x.start()
    entry_barrier(count, peer)

    def off_copy(step, block_at):
        _, m, g = peer(step)
        return pltpu.make_async_remote_copy(
            off, off_all.at[block_at], off_send.at[step], off_recv.at[block_at], (m, g), MESH)

    def aux_copy(step, block_at):
        _, m, g = peer(step)
        return pltpu.make_async_remote_copy(
            aux, aux_out.at[block_at], aux_send.at[step], aux_recv.at[block_at], (m, g), MESH)

    def x_copy(step, row_at):
        _, m, g = peer(step)
        block = g * members + m
        return pltpu.make_async_remote_copy(
            ens.at[:, pl.ds(pl.multiple_of(block * links, links), links)],
            x_out.at[row_at], x_send.at[step], x_recv.at[row_at], (m, g), MESH)

    def pick_copy(step, row_at):
        _, m, g = peer(step)
        return pltpu.make_async_remote_copy(
            own_picks, picks_out.at[row_at], pick_send.at[step], pick_recv.at[row_at], (m, g), MESH)

    def send_small(step, carry):
        off_copy(step, my_block).start()
        return carry

    def send_x(step, carry):
        x_copy(step, me).start()
        aux_copy(step, my_block).start()
        return carry

    def wait_off(step, carry):
        _, m, g = peer(step)
        off_copy(step, g * members + m).wait_recv()
        return carry

    lax.fori_loop(1, count, send_small, 0)
    own_off.wait()
    lax.fori_loop(1, count, wait_off, 0)

    group = 128 // obs

    def pick(chunk, carry):
        parts = []
        for at in range(group):
            block = chunk * group + at
            column = off_all[block][:, :1]
            hot = (lax.broadcasted_iota(jnp.int32, (obs, links), 1) == column).astype(F32).astype(BF16)
            values = ens[:, pl.ds(pl.multiple_of(block * links, links), links)]
            parts.append(lax.dot_general(values, hot, (((1,), (1,)), ((), ())), preferred_element_type=F32))
        own_picks[:, pl.ds(pl.multiple_of(chunk * 128, 128), 128)] = jnp.concatenate(parts, axis=1).astype(BF16)
        return carry

    lax.fori_loop(0, count // group, pick, 0)
    own_pick = pltpu.make_async_copy(own_picks, picks_out.at[me], local_sem.at[3])
    own_pick.start()

    def send_pick(step, carry):
        pick_copy(step, me).start()
        return carry

    lax.fori_loop(1, count, send_pick, 0)
    lax.fori_loop(1, count, send_x, 0)

    def finish(step, carry):
        other, m, g = peer(step)
        block = g * members + m
        pick_copy(step, other).wait()
        aux_copy(step, block).wait()
        x_copy(step, other).wait()
        off_copy(step, block).wait_send()
        return carry

    lax.fori_loop(1, count, finish, 0)
    own_aux.wait()
    own_x.wait()
    own_pick.wait()


def scatter_kernel(members, regions, x, out, send, recv, local_sem):
    count, me, my_block, peer = peers(members, regions)
    links = x.shape[2]

    def columns(block):
        return out.at[:, pl.ds(pl.multiple_of(block * links, links), links)]

    own = pltpu.make_async_copy(x.at[me], columns(my_block), local_sem)
    own.start()
    entry_barrier(count, peer)

    def copy(step, block_at):
        other, m, g = peer(step)
        return pltpu.make_async_remote_copy(
            x.at[other], columns(block_at), send.at[step], recv.at[block_at], (m, g), MESH)

    def start(step, carry):
        copy(step, my_block).start()
        return carry

    def finish(step, carry):
        _, m, g = peer(step)
        copy(step, g * members + m).wait()
        return carry

    lax.fori_loop(1, count, start, 0)
    lax.fori_loop(1, count, finish, 0)
    own.wait()


def halves(value):
    high = value.astype(BF16)
    return high, (value - high.astype(F32)).astype(BF16)


def mix_kernel(picks, values, variance, x, out, a_f, a_h, a_l, w_f, w_h, w_l, z_f):
    size = picks.shape[0]
    width = min(256, size)
    dot = functools.partial(jnp.dot, preferred_element_type=F32)
    exact = functools.partial(jnp.dot, preferred_element_type=F32, precision=lax.Precision.HIGHEST)

    def each(total, body):
        def step(chunk, carry):
            body(pl.ds(pl.multiple_of(chunk * width, width), width), chunk * width)
            return carry

        lax.fori_loop(0, total // width, step, 0)

    def eye(start, columns):
        rows = lax.broadcasted_iota(jnp.int32, (size, columns), 0)
        return (rows == lax.broadcasted_iota(jnp.int32, (size, columns), 1) + start).astype(F32)

    picked = picks[...].astype(F32)
    center = jnp.sum(picked, axis=0, keepdims=True) / size
    anomaly = picked - center
    innovation = values[...] - center
    spread = jnp.sum(anomaly * anomaly, axis=0, keepdims=True) / (size - 1.0) + variance[...]
    lift = jnp.sum(innovation * innovation, axis=1, keepdims=True) / jnp.sum(spread, axis=1, keepdims=True)
    inflation = jnp.sqrt(lift)
    weight = 1.0 / ((size - 1.0) * variance[...])
    column = jnp.sum(anomaly * (lift * weight * innovation), axis=1, keepdims=True)
    scaled = anomaly * jnp.sqrt(lift * weight)
    flipped = scaled.T
    for start in range(0, size, width):
        chunk = slice(start, start + width)
        a_f[:, chunk] = exact(scaled, flipped[:, chunk]) + eye(start, width)
    a_h[...], a_l[...] = halves(a_f[...])

    def square(cols, start):
        z_f[:, cols] = (
            dot(a_h[...], a_h[:, cols]) + dot(a_l[...], a_h[:, cols]) + dot(a_h[...], a_l[:, cols])
        )

    each(size, square)
    norm = jnp.max(jnp.sum(jnp.abs(z_f[:, :size]), axis=1, keepdims=True))
    plain = jnp.max(jnp.sum(jnp.abs(a_f[...]), axis=1, keepdims=True))
    top = jnp.minimum(jnp.sqrt(norm) * 1.01, plain * 1.0001)
    gentle = top < 400.0

    def opening(square_of):
        start = 2.0 / (1.0 + top)
        ratio = (top - 1.0) / (top + 1.0)
        scale = 2.0 / (2.0 - ratio * ratio)
        w_f[:, :size] = scale * (2.0 * start * a_f[...] - start * start * square_of)
        w_f[:, size:] = scale * start * (2.0 * eye(0, size) - start * a_f[...])
        return ratio * ratio / (2.0 - ratio * ratio)

    def refine(product, tolerance, limit, bound):
        def going(state):
            return jnp.logical_and(state[0] > tolerance, state[1] < limit)

        def step(state):
            bound, count = state
            scale = 2.0 / (2.0 - bound * bound)
            product(scale)
            w_f[...] = z_f[...]
            return bound * bound / (2.0 - bound * bound), count + 1

        lax.while_loop(going, step, (bound, 0))

    @pl.when(gentle)
    def _():
        bound = opening(z_f[:, :size])

        def product(scale):
            w_h[...], w_l[...] = halves(w_f[...])

            def body(cols, start):
                z_f[:, cols] = scale * (2.0 * w_f[:, cols] - (
                    dot(w_h[:, :size], w_h[:, cols]) + dot(w_l[:, :size], w_h[:, cols]) + dot(w_h[:, :size], w_l[:, cols])
                ))

            each(2 * size, body)

        refine(product, 0.01, 24, bound)
        w_h[:, size:], w_l[:, size:] = halves(w_f[:, size:])

        def residual(cols, start):
            right = pl.ds(pl.multiple_of(size + start, width), width)
            w_h[:, cols] = (eye(start, width) - (
                dot(a_h[...], w_h[:, right]) + dot(a_l[...], w_h[:, right]) + dot(a_h[...], w_l[:, right])
            )).astype(BF16)

        def correct(cols, start):
            right = pl.ds(pl.multiple_of(size + start, width), width)
            z_f[:, cols] = w_f[:, right] + dot(w_h[:, size:], w_h[:, cols])

        each(size, residual)
        each(size, correct)

    @pl.when(jnp.logical_not(gentle))
    def _():
        def square_exact(cols, start):
            z_f[:, cols] = exact(a_f[...], a_f[:, cols])

        each(size, square_exact)
        bound = opening(z_f[:, :size])

        def product(scale):
            def body(cols, start):
                z_f[:, cols] = scale * (2.0 * w_f[:, cols] - exact(w_f[:, :size], w_f[:, cols]))

            each(2 * size, body)

        refine(product, 0.01, 40, bound)

        def again(count, carry):
            def residual(cols, start):
                right = pl.ds(pl.multiple_of(size + start, width), width)
                w_f[:, cols] = eye(start, width) - exact(a_f[...], w_f[:, right])

            def correct(cols, start):
                right = pl.ds(pl.multiple_of(size + start, width), width)
                z_f[:, cols] = w_f[:, right] + exact(w_f[:, size:], w_f[:, cols])

            each(size, residual)
            each(size, correct)
            w_f[:, size:] = z_f[:, :size]
            return carry

        lax.fori_loop(0, 2, again, 0)

    inverse = z_f[:, :size]
    gain = jnp.sum(inverse * column, axis=0, keepdims=True)
    mixing = 0.5 * inflation * (eye(0, size) + inverse) + (gain + (1.0 - inflation) / size)
    a_h[...], a_l[...] = halves(mixing)

    def apply(cols, start):
        out[:, cols] = (dot(a_h[...], x[:, cols]) + dot(a_l[...], x[:, cols])).astype(BF16)

    each(x.shape[1], apply)


def local(ensemble, obs_offset, observed, obs_var):
    members = lax.axis_size("member")
    regions = lax.axis_size("region")
    count = members * regions
    own = ensemble.shape[0]
    size = own * count
    links = ensemble.shape[1] // count
    obs = obs_offset.shape[2]
    total = count * obs
    offsets = jnp.broadcast_to(obs_offset.reshape(obs, 1), (obs, 128))
    aux = jnp.zeros((8, 128), F32).at[0, :obs].set(observed.reshape(-1)).at[1, :obs].set(obs_var.reshape(-1))
    vmem = pl.BlockSpec(memory_space=pltpu.VMEM)
    sems = pltpu.SemaphoreType.DMA((count,))
    x, picks, every_aux = pl.pallas_call(
        functools.partial(gather_kernel, members, regions),
        out_shape=(
            jax.ShapeDtypeStruct((count, own, links), BF16),
            jax.ShapeDtypeStruct((count, own, total), BF16),
            jax.ShapeDtypeStruct((count, 8, 128), F32),
        ),
        in_specs=[vmem] * 3,
        out_specs=(vmem,) * 3,
        scratch_shapes=[
            pltpu.VMEM((count, obs, 128), jnp.int32),
            pltpu.VMEM((own, total), BF16),
        ] + [sems] * 8 + [pltpu.SemaphoreType.DMA((4,))],
        compiler_params=pltpu.CompilerParams(
            collective_id=0, has_side_effects=True, vmem_limit_bytes=VMEM_LIMIT),
    )(ensemble, offsets, aux)
    values = every_aux[:, 0, :obs].reshape(1, total)
    variance = every_aux[:, 1, :obs].reshape(1, total)
    mixed = pl.pallas_call(
        mix_kernel,
        out_shape=jax.ShapeDtypeStruct((size, links), BF16),
        in_specs=[vmem] * 4,
        out_specs=vmem,
        scratch_shapes=[
            pltpu.VMEM((size, size), F32),
            pltpu.VMEM((size, size), BF16),
            pltpu.VMEM((size, size), BF16),
            pltpu.VMEM((size, 2 * size), F32),
            pltpu.VMEM((size, 2 * size), BF16),
            pltpu.VMEM((size, 2 * size), BF16),
            pltpu.VMEM((size, 2 * size), F32),
        ],
        compiler_params=pltpu.CompilerParams(vmem_limit_bytes=VMEM_LIMIT),
    )(picks.reshape(size, total), values, variance, x.reshape(size, links))
    return pl.pallas_call(
        functools.partial(scatter_kernel, members, regions),
        out_shape=jax.ShapeDtypeStruct(ensemble.shape, BF16),
        in_specs=[vmem],
        out_specs=vmem,
        scratch_shapes=[sems, sems, pltpu.SemaphoreType.DMA],
        compiler_params=pltpu.CompilerParams(
            collective_id=1, has_side_effects=True, vmem_limit_bytes=VMEM_LIMIT),
    )(mixed.reshape(count, own, links))


def solution(mesh):
    return jax.shard_map(
        local,
        mesh=mesh,
        in_specs=(
            P(("member", "region"), None),
            P("region", "member", None),
            P("region", "member", None),
            P("region", "member", None),
        ),
        out_specs=P(("member", "region"), None),
        check_vma=False,
    )
```

```python
import functools

import jax
import jax.numpy as jnp
from jax import lax
from jax.experimental import pallas as pl
from jax.experimental.pallas import tpu as pltpu
from jax.sharding import PartitionSpec as P

MESH = pl.DeviceIdType.MESH
F32 = jnp.float32
BF16 = jnp.bfloat16
VMEM_LIMIT = 56 * 1024 * 1024


def peers(members, regions):
    count = members * regions
    own_member, own_region = lax.axis_index("member"), lax.axis_index("region")
    me = own_member * regions + own_region

    def peer(step):
        other = (me + step) % count
        return other, other // regions, other % regions

    return count, me, own_region * members + own_member, peer


def entry_barrier(count, peer):
    barrier = pltpu.get_barrier_semaphore()

    def greet(step, carry):
        _, m, g = peer(step)
        pl.semaphore_signal(barrier, inc=1, device_id=(m, g), device_id_type=MESH)
        return carry

    lax.fori_loop(1, count, greet, 0)
    pl.semaphore_wait(barrier, count - 1)


def halves(value):
    high = value.astype(BF16)
    return high, (value - high.astype(F32)).astype(BF16)


def eye(size, start, columns):
    rows = lax.broadcasted_iota(jnp.int32, (size, columns), 0)
    return (rows == lax.broadcasted_iota(jnp.int32, (size, columns), 1) + start).astype(F32)


def each(total, width, body):
    def step(chunk, carry):
        body(pl.ds(pl.multiple_of(chunk * width, width), width), chunk * width)
        return carry

    lax.fori_loop(0, total // width, step, 0)


dot = functools.partial(jnp.dot, preferred_element_type=F32)
exact = functools.partial(jnp.dot, preferred_element_type=F32, precision=lax.Precision.HIGHEST)


def dot_nt(left, right):
    return lax.dot_general(left, right, (((1,), (1,)), ((), ())), preferred_element_type=F32)


def spectrum_bound(squared, plain):
    norm = jnp.max(jnp.sum(jnp.abs(squared), axis=1, keepdims=True), axis=0, keepdims=True)
    other = jnp.max(jnp.sum(jnp.abs(plain), axis=1, keepdims=True), axis=0, keepdims=True)
    return jnp.minimum(jnp.sqrt(norm) * 1.01, other * 1.0001)


def opening(size, top, a_f, squared, w_f):
    start = 2.0 / (1.0 + top)
    ratio = (top - 1.0) / (top + 1.0)
    scale = 2.0 / (2.0 - ratio * ratio)
    w_f[:, :size] = scale * (2.0 * start * a_f[...] - start * start * squared)
    w_f[:, size:] = scale * start * (2.0 * eye(size, 0, size) - start * a_f[...])
    return ratio * ratio / (2.0 - ratio * ratio)


def gather_kernel(members, regions, ens, off, aux, x_out, a_f, inv, col, scal, off_all, aux_all, own_picks, picks,
                  rows, s_h, s_l, a_h, a_l, w_f, w_h, w_l,
                  off_send, off_recv, aux_send, aux_recv, x_send, x_recv, one_send, one_recv, two_send, two_recv,
                  local_sem):
    count, me, my_block, peer = peers(members, regions)
    my_m, my_g = lax.axis_index("member"), lax.axis_index("region")
    links = x_out.shape[2]
    obs = off.shape[0]
    total = own_picks.shape[1]
    size = a_f.shape[0]
    width = min(256, size)
    group = 128 // obs

    own_off = pltpu.make_async_copy(off, off_all.at[my_block], local_sem.at[0])
    own_aux = pltpu.make_async_copy(aux, aux_all.at[my_block], local_sem.at[1])
    own_x = pltpu.make_async_copy(
        ens.at[:, pl.ds(pl.multiple_of(my_block * links, links), links)], x_out.at[me], local_sem.at[2])
    own_off.start()
    own_aux.start()
    own_x.start()
    entry_barrier(count, peer)

    def off_copy(step, block_at):
        _, m, g = peer(step)
        return pltpu.make_async_remote_copy(
            off, off_all.at[block_at], off_send.at[step], off_recv.at[block_at], (m, g), MESH)

    def aux_copy(step, block_at):
        _, m, g = peer(step)
        return pltpu.make_async_remote_copy(
            aux, aux_all.at[block_at], aux_send.at[step], aux_recv.at[block_at], (m, g), MESH)

    def x_copy(m, g, row_at):
        block = g * members + m
        return pltpu.make_async_remote_copy(
            ens.at[:, pl.ds(pl.multiple_of(block * links, links), links)],
            x_out.at[row_at], x_send.at[m * regions + g], x_recv.at[row_at], (m, g), MESH)

    def one_copy(m, m_at):
        return pltpu.make_async_remote_copy(
            own_picks, picks.at[m_at, my_g], one_send.at[m], one_recv.at[m_at], (m, my_g), MESH)

    def two_copy(g, g_at):
        return pltpu.make_async_remote_copy(
            picks.at[:, my_g], picks.at[:, g_at], two_send.at[g], two_recv.at[g_at], (my_m, g), MESH)

    def loop(low, high, body):
        def step(at, carry):
            body(at)
            return carry

        lax.fori_loop(low, high, step, 0)

    def next_m(step):
        return (my_m + step) % members

    def next_g(step):
        return (my_g + step) % regions

    loop(1, count, lambda step: off_copy(step, my_block).start())
    loop(1, count, lambda step: aux_copy(step, my_block).start())
    loop(1, members, lambda step: x_copy(next_m(step), my_g, me).start())
    own_off.wait()

    def wait_off(step):
        _, m, g = peer(step)
        off_copy(step, g * members + m).wait_recv()

    loop(1, count, wait_off)

    def pick(chunk):
        parts = []
        for at in range(group):
            block = chunk * group + at
            column = off_all[block][:, :1]
            hot = (lax.broadcasted_iota(jnp.int32, (obs, links), 1) == column).astype(F32).astype(BF16)
            values = ens[:, pl.ds(pl.multiple_of(block * links, links), links)]
            parts.append(dot_nt(values, hot))
        own_picks[:, pl.ds(pl.multiple_of(chunk * 128, 128), 128)] = jnp.concatenate(parts, axis=1).astype(BF16)

    loop(0, count // group, pick)
    own_pick = pltpu.make_async_copy(own_picks, picks.at[my_m, my_g], local_sem.at[3])
    own_pick.start()
    loop(1, members, lambda step: one_copy(next_m(step), my_m).start())
    own_pick.wait()
    loop(1, members, lambda step: one_copy(next_m(step), next_m(step)).wait_recv())
    loop(1, regions, lambda step: two_copy(next_g(step), my_g).start())

    def send_rest(step):
        x_copy((my_m + step // (regions - 1)) % members, next_g(1 + step % (regions - 1)), me).start()

    loop(0, members * (regions - 1), send_rest)
    own_aux.wait()

    def wait_aux(step):
        _, m, g = peer(step)
        aux_copy(step, g * members + m).wait_recv()

    loop(1, count, wait_aux)
    lane = lax.broadcasted_iota(jnp.int32, (8, 128), 1) // obs

    def spread_aux(chunk):
        value = jnp.zeros((8, 128), F32)
        for at in range(group):
            value = jnp.where(lane == at, aux_all[chunk * group + at], value)
        rows[:, pl.ds(pl.multiple_of(chunk * 128, 128), 128)] = value

    loop(0, count // group, spread_aux)
    loop(1, regions, lambda step: two_copy(next_g(step), next_g(step)).wait_recv())

    values, variance = rows[0:1, :], rows[1:2, :]
    picked = picks[...].astype(F32).reshape(size, total)
    center = jnp.sum(picked, axis=0, keepdims=True) / size
    anomaly = picked - center
    innovation = values - center
    spread = jnp.sum(anomaly * anomaly, axis=0, keepdims=True) / (size - 1.0) + variance
    lift = jnp.sum(innovation * innovation, axis=1, keepdims=True) / jnp.sum(spread, axis=1, keepdims=True)
    weight = 1.0 / ((size - 1.0) * variance)
    column = jnp.sum(anomaly * (lift * weight * innovation), axis=1, keepdims=True)
    col[...] = jnp.broadcast_to(column, col.shape)
    s_h[...], s_l[...] = halves(anomaly * jnp.sqrt(lift * weight))

    def products(cols, start):
        a_f[:, cols] = eye(size, start, width) + (
            dot_nt(s_h[...], s_h[cols, :]) + dot_nt(s_l[...], s_h[cols, :]) + dot_nt(s_h[...], s_l[cols, :])
        )

    each(size, width, products)
    a_h[...], a_l[...] = halves(a_f[...])

    def square(cols, start):
        inv[:, cols] = (
            dot(a_h[...], a_h[:, cols]) + dot(a_l[...], a_h[:, cols]) + dot(a_h[...], a_l[:, cols])
        )

    each(size, width, square)
    top = spectrum_bound(inv[...], a_f[...])
    scal[...] = jnp.where(lax.broadcasted_iota(jnp.int32, scal.shape, 0) == 0, lift, top)
    bound = opening(size, top, a_f, inv[...], w_f)

    def full_step(count, bound):
        scale = 2.0 / (2.0 - bound * bound)
        w_h[...], w_l[...] = halves(w_f[...])

        def body(cols, start):
            w_f[:, cols] = scale * (2.0 * w_f[:, cols] - (
                dot(w_h[:, :size], w_h[:, cols]) + dot(w_l[:, :size], w_h[:, cols]) + dot(w_h[:, :size], w_l[:, cols])
            ))

        each(2 * size, width, body)
        return bound * bound / (2.0 - bound * bound)

    bound = lax.fori_loop(0, 3, full_step, bound)
    scale = 2.0 / (2.0 - bound * bound)
    w_h[...] = w_f[...].astype(BF16)

    def last_step(cols, start):
        right = pl.ds(pl.multiple_of(size + start, width), width)
        w_f[:, right] = scale * (2.0 * w_f[:, right] - dot(w_h[:, :size], w_h[:, right]))

    each(size, width, last_step)
    w_h[:, size:], w_l[:, size:] = halves(w_f[:, size:])

    def correct(cols, start):
        right = pl.ds(pl.multiple_of(size + start, width), width)
        rest = eye(size, start, width) - (
            dot(a_h[...], w_h[:, right]) + dot(a_l[...], w_h[:, right]) + dot(a_h[...], w_l[:, right])
        )
        inv[:, cols] = w_f[:, right] + dot(w_h[:, size:], rest.astype(BF16))

    each(size, width, correct)

    def finish_all(step):
        off_copy(step, my_block).wait_send()
        aux_copy(step, my_block).wait_send()
        other, m, g = peer(step)
        x_copy(m, g, other).wait()

    loop(1, count, finish_all)
    loop(1, members, lambda step: one_copy(next_m(step), my_m).wait_send())
    loop(1, regions, lambda step: two_copy(next_g(step), my_g).wait_send())
    own_x.wait()


def scatter_kernel(members, regions, x, out, send, recv, local_sem):
    count, me, my_block, peer = peers(members, regions)
    links = x.shape[2]

    def columns(block):
        return out.at[:, pl.ds(pl.multiple_of(block * links, links), links)]

    own = pltpu.make_async_copy(x.at[me], columns(my_block), local_sem)
    own.start()
    entry_barrier(count, peer)

    def copy(step, block_at):
        other, m, g = peer(step)
        return pltpu.make_async_remote_copy(
            x.at[other], columns(block_at), send.at[step], recv.at[block_at], (m, g), MESH)

    def start(step, carry):
        copy(step, my_block).start()
        return carry

    def finish(step, carry):
        _, m, g = peer(step)
        copy(step, g * members + m).wait()
        return carry

    lax.fori_loop(1, count, start, 0)
    lax.fori_loop(1, count, finish, 0)
    own.wait()


def mix_kernel(col, scal, inv, x, a_any, out, a_f, m_h, m_l, w_f, z_f, sem):
    size = inv.shape[0]
    width = min(256, size)
    lift = scal[0:1, 0:1]
    inflation = jnp.sqrt(lift)
    column = col[:, :1]

    def finish(inverse):
        gain = jnp.sum(inverse * column, axis=0, keepdims=True)
        m_h[...], m_l[...] = halves(
            0.5 * inflation * (eye(size, 0, size) + inverse) + (gain + (1.0 - inflation) / size))

    gentle = jnp.max(scal[1:2, :]) < 150.0

    @pl.when(gentle)
    def _():
        finish(inv[...])

    @pl.when(jnp.logical_not(gentle))
    def _():
        fetch = pltpu.make_async_copy(a_any, a_f, sem)
        fetch.start()
        fetch.wait()

        def square_exact(cols, start):
            z_f[:, cols] = exact(a_f[...], a_f[:, cols])

        each(size, width, square_exact)
        top = jnp.max(spectrum_bound(z_f[:, :size], a_f[...]))
        bound = opening(size, top, a_f, z_f[:, :size], w_f)

        def going(state):
            return jnp.logical_and(state[0] > 0.01, state[1] < 40)

        def step(state):
            bound, count = state
            scale = 2.0 / (2.0 - bound * bound)

            def body(cols, start):
                z_f[:, cols] = scale * (2.0 * w_f[:, cols] - exact(w_f[:, :size], w_f[:, cols]))

            each(2 * size, width, body)
            w_f[...] = z_f[...]
            return bound * bound / (2.0 - bound * bound), count + 1

        lax.while_loop(going, step, (bound, 0))

        def again(count, carry):
            def residual(cols, start):
                right = pl.ds(pl.multiple_of(size + start, width), width)
                w_f[:, cols] = eye(size, start, width) - exact(a_f[...], w_f[:, right])

            def correct(cols, start):
                right = pl.ds(pl.multiple_of(size + start, width), width)
                z_f[:, cols] = w_f[:, right] + exact(w_f[:, size:], w_f[:, cols])

            each(size, width, residual)
            each(size, width, correct)
            w_f[:, size:] = z_f[:, :size]
            return carry

        lax.fori_loop(0, 2, again, 0)
        finish(z_f[:, :size])

    def apply(cols, start):
        out[:, cols] = (dot(m_h[...], x[:, cols]) + dot(m_l[...], x[:, cols])).astype(BF16)

    each(x.shape[1], width, apply)


def local(ensemble, obs_offset, observed, obs_var):
    members = lax.axis_size("member")
    regions = lax.axis_size("region")
    count = members * regions
    own = ensemble.shape[0]
    size = own * count
    links = ensemble.shape[1] // count
    obs = obs_offset.shape[2]
    total = count * obs
    offsets = jnp.broadcast_to(obs_offset.reshape(obs, 1), (obs, 128))
    aux = jnp.tile(jnp.concatenate([observed.reshape(1, obs), obs_var.reshape(1, obs)], axis=0), (4, 128 // obs))
    vmem = pl.BlockSpec(memory_space=pltpu.VMEM)
    sems = pltpu.SemaphoreType.DMA((count,))
    member_sems = pltpu.SemaphoreType.DMA((members,))
    region_sems = pltpu.SemaphoreType.DMA((regions,))
    x, system, inverse, column, scalars = pl.pallas_call(
        functools.partial(gather_kernel, members, regions),
        out_shape=(
            jax.ShapeDtypeStruct((count, own, links), BF16),
            jax.ShapeDtypeStruct((size, size), F32),
            jax.ShapeDtypeStruct((size, size), F32),
            jax.ShapeDtypeStruct((size, 128), F32),
            jax.ShapeDtypeStruct((8, 128), F32),
        ),
        in_specs=[vmem] * 3,
        out_specs=(vmem,) * 5,
        scratch_shapes=[
            pltpu.VMEM((count, obs, 128), jnp.int32),
            pltpu.VMEM((count, 8, 128), F32),
            pltpu.VMEM((own, total), BF16),
            pltpu.VMEM((members, regions, own, total), BF16),
            pltpu.VMEM((8, total), F32),
            pltpu.VMEM((size, total), BF16),
            pltpu.VMEM((size, total), BF16),
            pltpu.VMEM((size, size), BF16),
            pltpu.VMEM((size, size), BF16),
            pltpu.VMEM((size, 2 * size), F32),
            pltpu.VMEM((size, 2 * size), BF16),
            pltpu.VMEM((size, 2 * size), BF16),
        ] + [sems] * 6 + [member_sems] * 2 + [region_sems] * 2 + [pltpu.SemaphoreType.DMA((4,))],
        compiler_params=pltpu.CompilerParams(
            collective_id=0, has_side_effects=True, vmem_limit_bytes=VMEM_LIMIT),
    )(ensemble, offsets, aux)
    mixed = pl.pallas_call(
        mix_kernel,
        out_shape=jax.ShapeDtypeStruct((size, links), BF16),
        in_specs=[vmem] * 4 + [pl.BlockSpec(memory_space=pl.ANY)],
        out_specs=vmem,
        scratch_shapes=[
            pltpu.VMEM((size, size), F32),
            pltpu.VMEM((size, size), BF16),
            pltpu.VMEM((size, size), BF16),
            pltpu.VMEM((size, 2 * size), F32),
            pltpu.VMEM((size, 2 * size), F32),
            pltpu.SemaphoreType.DMA,
        ],
        compiler_params=pltpu.CompilerParams(vmem_limit_bytes=VMEM_LIMIT),
    )(column, scalars, inverse, x.reshape(size, links), system)
    return pl.pallas_call(
        functools.partial(scatter_kernel, members, regions),
        out_shape=jax.ShapeDtypeStruct(ensemble.shape, BF16),
        in_specs=[vmem],
        out_specs=vmem,
        scratch_shapes=[sems, sems, pltpu.SemaphoreType.DMA],
        compiler_params=pltpu.CompilerParams(
            collective_id=1, has_side_effects=True, vmem_limit_bytes=VMEM_LIMIT),
    )(mixed.reshape(count, own, links))


def solution(mesh):
    return jax.shard_map(
        local,
        mesh=mesh,
        in_specs=(
            P(("member", "region"), None),
            P("region", "member", None),
            P("region", "member", None),
            P("region", "member", None),
        ),
        out_specs=P(("member", "region"), None),
        check_vma=False,
    )
```

```python
import functools

import jax
import jax.numpy as jnp
from jax import lax
from jax.experimental import pallas as pl
from jax.experimental.pallas import tpu as pltpu
from jax.sharding import PartitionSpec as P

MESH = pl.DeviceIdType.MESH
F32 = jnp.float32
BF16 = jnp.bfloat16
MIB = 1024 * 1024


def peers(members, regions):
    count = members * regions
    own_member, own_region = lax.axis_index("member"), lax.axis_index("region")
    me = own_member * regions + own_region

    def peer(step):
        other = (me + step) % count
        return other, other // regions, other % regions

    return count, me, own_region * members + own_member, peer


def entry_barrier(count, peer):
    barrier = pltpu.get_barrier_semaphore()

    def greet(step, carry):
        _, m, g = peer(step)
        pl.semaphore_signal(barrier, inc=1, device_id=(m, g), device_id_type=MESH)
        return carry

    lax.fori_loop(1, count, greet, 0)
    pl.semaphore_wait(barrier, count - 1)


def halves(value):
    high = value.astype(BF16)
    return high, (value - high.astype(F32)).astype(BF16)


def eye(size, start, columns):
    rows = lax.broadcasted_iota(jnp.int32, (size, columns), 0)
    return (rows == lax.broadcasted_iota(jnp.int32, (size, columns), 1) + start).astype(F32)


def each(total, width, body):
    def step(chunk, carry):
        body(pl.ds(pl.multiple_of(chunk * width, width), width), chunk * width)
        return carry

    lax.fori_loop(0, total // width, step, 0)


dot = functools.partial(jnp.dot, preferred_element_type=F32)
exact = functools.partial(jnp.dot, preferred_element_type=F32, precision=lax.Precision.HIGHEST)


def dot_nt(left, right):
    return lax.dot_general(left, right, (((1,), (1,)), ((), ())), preferred_element_type=F32)


def spectrum_bound(squared, plain):
    norm = jnp.max(jnp.sum(jnp.abs(squared), axis=1, keepdims=True), axis=0, keepdims=True)
    other = jnp.max(jnp.sum(jnp.abs(plain), axis=1, keepdims=True), axis=0, keepdims=True)
    return jnp.minimum(jnp.sqrt(norm) * 1.01, other * 1.0001)


def opening(size, top, a_f, squared, w_f):
    start = 2.0 / (1.0 + top)
    ratio = (top - 1.0) / (top + 1.0)
    scale = 2.0 / (2.0 - ratio * ratio)
    w_f[:, :size] = scale * (2.0 * start * a_f[...] - start * start * squared)
    w_f[:, size:] = scale * start * (2.0 * eye(size, 0, size) - start * a_f[...])
    return ratio * ratio / (2.0 - ratio * ratio)


def gather_kernel(members, regions, ens, off, aux, x_out, a_f, inv, col, scal, off_all, aux_all, own_picks, picks,
                  rows, s_h, s_l, a_h, a_l, w_f, w_h, w_l,
                  off_send, off_recv, aux_send, aux_recv, x_send, x_recv, one_send, one_recv, two_send, two_recv,
                  local_sem):
    count, me, my_block, peer = peers(members, regions)
    my_m, my_g = lax.axis_index("member"), lax.axis_index("region")
    links = x_out.shape[2]
    obs = off.shape[0]
    total = own_picks.shape[1]
    size = a_f.shape[0]
    width = min(256, size)
    group = 128 // obs

    own_off = pltpu.make_async_copy(off, off_all.at[my_block], local_sem.at[0])
    own_aux = pltpu.make_async_copy(aux, aux_all.at[my_block], local_sem.at[1])
    own_x = pltpu.make_async_copy(
        ens.at[:, pl.ds(pl.multiple_of(my_block * links, links), links)], x_out.at[me], local_sem.at[2])
    own_off.start()
    own_aux.start()
    own_x.start()
    entry_barrier(count, peer)

    def off_copy(step, block_at):
        _, m, g = peer(step)
        return pltpu.make_async_remote_copy(
            off, off_all.at[block_at], off_send.at[step], off_recv.at[block_at], (m, g), MESH)

    def aux_copy(step, block_at):
        _, m, g = peer(step)
        return pltpu.make_async_remote_copy(
            aux, aux_all.at[block_at], aux_send.at[step], aux_recv.at[block_at], (m, g), MESH)

    def x_copy(m, g, row_at):
        block = g * members + m
        return pltpu.make_async_remote_copy(
            ens.at[:, pl.ds(pl.multiple_of(block * links, links), links)],
            x_out.at[row_at], x_send.at[m * regions + g], x_recv.at[row_at], (m, g), MESH)

    def one_copy(m, m_at):
        return pltpu.make_async_remote_copy(
            own_picks, picks.at[m_at, my_g], one_send.at[m], one_recv.at[m_at], (m, my_g), MESH)

    def two_copy(g, g_at):
        return pltpu.make_async_remote_copy(
            picks.at[:, my_g], picks.at[:, g_at], two_send.at[g], two_recv.at[g_at], (my_m, g), MESH)

    def loop(low, high, body):
        def step(at, carry):
            body(at)
            return carry

        lax.fori_loop(low, high, step, 0)

    def next_m(step):
        return (my_m + step) % members

    def next_g(step):
        return (my_g + step) % regions

    loop(1, count, lambda step: off_copy(step, my_block).start())
    loop(1, count, lambda step: aux_copy(step, my_block).start())
    own_off.wait()

    def wait_off(step):
        _, m, g = peer(step)
        off_copy(step, g * members + m).wait_recv()

    loop(1, count, wait_off)

    def pick(chunk):
        parts = []
        for at in range(group):
            block = chunk * group + at
            column = off_all[block][:, :1]
            hot = (lax.broadcasted_iota(jnp.int32, (obs, links), 1) == column).astype(F32).astype(BF16)
            values = ens[:, pl.ds(pl.multiple_of(block * links, links), links)]
            parts.append(dot_nt(values, hot))
        own_picks[:, pl.ds(pl.multiple_of(chunk * 128, 128), 128)] = jnp.concatenate(parts, axis=1).astype(BF16)

    loop(0, count // group, pick)
    own_pick = pltpu.make_async_copy(own_picks, picks.at[my_m, my_g], local_sem.at[3])
    own_pick.start()
    loop(1, members, lambda step: one_copy(next_m(step), my_m).start())
    loop(1, members, lambda step: x_copy(next_m(step), my_g, me).start())
    own_pick.wait()
    loop(1, members, lambda step: one_copy(next_m(step), next_m(step)).wait_recv())
    loop(1, regions, lambda step: two_copy(next_g(step), my_g).start())

    def send_rest(step):
        x_copy((my_m + step // (regions - 1)) % members, next_g(1 + step % (regions - 1)), me).start()

    loop(0, members * (regions - 1), send_rest)
    own_aux.wait()

    def wait_aux(step):
        _, m, g = peer(step)
        aux_copy(step, g * members + m).wait_recv()

    loop(1, count, wait_aux)
    lane = lax.broadcasted_iota(jnp.int32, (8, 128), 1) // obs

    def spread_aux(chunk):
        value = jnp.zeros((8, 128), F32)
        for at in range(group):
            value = jnp.where(lane == at, aux_all[chunk * group + at], value)
        rows[:, pl.ds(pl.multiple_of(chunk * 128, 128), 128)] = value

    loop(0, count // group, spread_aux)
    loop(1, regions, lambda step: two_copy(next_g(step), next_g(step)).wait_recv())

    values, variance = rows[0:1, :], rows[1:2, :]
    picked = picks[...].astype(F32).reshape(size, total)
    center = jnp.sum(picked, axis=0, keepdims=True) / size
    anomaly = picked - center
    innovation = values - center
    spread = jnp.sum(anomaly * anomaly, axis=0, keepdims=True) / (size - 1.0) + variance
    lift = jnp.sum(innovation * innovation, axis=1, keepdims=True) / jnp.sum(spread, axis=1, keepdims=True)
    weight = 1.0 / ((size - 1.0) * variance)
    column = jnp.sum(anomaly * (lift * weight * innovation), axis=1, keepdims=True)
    col[...] = jnp.broadcast_to(column, col.shape)
    s_h[...], s_l[...] = halves(anomaly * jnp.sqrt(lift * weight))

    def products(cols, start):
        a_f[:, cols] = eye(size, start, width) + (
            dot_nt(s_h[...], s_h[cols, :]) + dot_nt(s_l[...], s_h[cols, :]) + dot_nt(s_h[...], s_l[cols, :])
        )

    each(size, width, products)
    a_h[...], a_l[...] = halves(a_f[...])

    def square(cols, start):
        inv[:, cols] = (
            dot(a_h[...], a_h[:, cols]) + dot(a_l[...], a_h[:, cols]) + dot(a_h[...], a_l[:, cols])
        )

    each(size, width, square)
    top = spectrum_bound(inv[...], a_f[...])
    scal[...] = jnp.where(lax.broadcasted_iota(jnp.int32, scal.shape, 0) == 0, lift, top)
    bound = opening(size, top, a_f, inv[...], w_f)

    def full_step(count, bound):
        scale = 2.0 / (2.0 - bound * bound)
        w_h[...], w_l[...] = halves(w_f[...])

        def body(cols, start):
            w_f[:, cols] = scale * (2.0 * w_f[:, cols] - (
                dot(w_h[:, :size], w_h[:, cols]) + dot(w_l[:, :size], w_h[:, cols]) + dot(w_h[:, :size], w_l[:, cols])
            ))

        each(2 * size, width, body)
        return bound * bound / (2.0 - bound * bound)

    bound = lax.fori_loop(0, 3, full_step, bound)
    scale = 2.0 / (2.0 - bound * bound)
    w_h[...] = w_f[...].astype(BF16)

    def last_step(cols, start):
        right = pl.ds(pl.multiple_of(size + start, width), width)
        w_f[:, right] = scale * (2.0 * w_f[:, right] - dot(w_h[:, :size], w_h[:, right]))

    each(size, width, last_step)
    w_h[:, size:], w_l[:, size:] = halves(w_f[:, size:])

    def correct(cols, start):
        right = pl.ds(pl.multiple_of(size + start, width), width)
        rest = eye(size, start, width) - (
            dot(a_h[...], w_h[:, right]) + dot(a_l[...], w_h[:, right]) + dot(a_h[...], w_l[:, right])
        )
        inv[:, cols] = w_f[:, right] + dot(w_h[:, size:], rest.astype(BF16))

    each(size, width, correct)

    def finish_all(step):
        off_copy(step, my_block).wait_send()
        aux_copy(step, my_block).wait_send()
        other, m, g = peer(step)
        x_copy(m, g, other).wait()

    loop(1, count, finish_all)
    loop(1, members, lambda step: one_copy(next_m(step), my_m).wait_send())
    loop(1, regions, lambda step: two_copy(next_g(step), my_g).wait_send())
    own_x.wait()


def scatter_kernel(members, regions, x, out, send, recv, local_sem):
    count, me, my_block, peer = peers(members, regions)
    links = x.shape[2]

    def columns(block):
        return out.at[:, pl.ds(pl.multiple_of(block * links, links), links)]

    own = pltpu.make_async_copy(x.at[me], columns(my_block), local_sem)
    own.start()
    entry_barrier(count, peer)

    def copy(step, block_at):
        other, m, g = peer(step)
        return pltpu.make_async_remote_copy(
            x.at[other], columns(block_at), send.at[step], recv.at[block_at], (m, g), MESH)

    def start(step, carry):
        copy(step, my_block).start()
        return carry

    def finish(step, carry):
        _, m, g = peer(step)
        copy(step, g * members + m).wait()
        return carry

    lax.fori_loop(1, count, start, 0)
    lax.fori_loop(1, count, finish, 0)
    own.wait()


def mix_kernel(col, scal, inv, x, a_any, out, a_f, m_h, m_l, w_f, z_f, sem):
    size = inv.shape[0]
    width = min(256, size)
    lift = scal[0:1, 0:1]
    inflation = jnp.sqrt(lift)
    column = col[:, :1]

    def finish(inverse):
        gain = jnp.sum(inverse * column, axis=0, keepdims=True)
        m_h[...], m_l[...] = halves(
            0.5 * inflation * (eye(size, 0, size) + inverse) + (gain + (1.0 - inflation) / size))

    gentle = jnp.max(scal[1:2, :]) < 150.0

    @pl.when(gentle)
    def _():
        finish(inv[...])

    @pl.when(jnp.logical_not(gentle))
    def _():
        fetch = pltpu.make_async_copy(a_any, a_f, sem)
        fetch.start()
        fetch.wait()

        def square_exact(cols, start):
            z_f[:, cols] = exact(a_f[...], a_f[:, cols])

        each(size, width, square_exact)
        top = jnp.max(spectrum_bound(z_f[:, :size], a_f[...]))
        bound = opening(size, top, a_f, z_f[:, :size], w_f)

        def going(state):
            return jnp.logical_and(state[0] > 0.01, state[1] < 40)

        def step(state):
            bound, count = state
            scale = 2.0 / (2.0 - bound * bound)

            def body(cols, start):
                z_f[:, cols] = scale * (2.0 * w_f[:, cols] - exact(w_f[:, :size], w_f[:, cols]))

            each(2 * size, width, body)
            w_f[...] = z_f[...]
            return bound * bound / (2.0 - bound * bound), count + 1

        lax.while_loop(going, step, (bound, 0))

        def again(count, carry):
            def residual(cols, start):
                right = pl.ds(pl.multiple_of(size + start, width), width)
                w_f[:, cols] = eye(size, start, width) - exact(a_f[...], w_f[:, right])

            def correct(cols, start):
                right = pl.ds(pl.multiple_of(size + start, width), width)
                z_f[:, cols] = w_f[:, right] + exact(w_f[:, size:], w_f[:, cols])

            each(size, width, residual)
            each(size, width, correct)
            w_f[:, size:] = z_f[:, :size]
            return carry

        lax.fori_loop(0, 2, again, 0)
        finish(z_f[:, :size])

    def apply(cols, start):
        out[:, cols] = (dot(m_h[...], x[:, cols]) + dot(m_l[...], x[:, cols])).astype(BF16)

    each(x.shape[1], width, apply)


def local(ensemble, obs_offset, observed, obs_var):
    members = lax.axis_size("member")
    regions = lax.axis_size("region")
    count = members * regions
    own = ensemble.shape[0]
    size = own * count
    links = ensemble.shape[1] // count
    obs = obs_offset.shape[2]
    total = count * obs
    offsets = jnp.broadcast_to(obs_offset.reshape(obs, 1), (obs, 128))
    aux = jnp.tile(jnp.concatenate([observed.reshape(1, obs), obs_var.reshape(1, obs)], axis=0), (4, 128 // obs))
    vmem = pl.BlockSpec(memory_space=pltpu.VMEM)
    sems = pltpu.SemaphoreType.DMA((count,))
    member_sems = pltpu.SemaphoreType.DMA((members,))
    region_sems = pltpu.SemaphoreType.DMA((regions,))
    x, system, inverse, column, scalars = pl.pallas_call(
        functools.partial(gather_kernel, members, regions),
        out_shape=(
            jax.ShapeDtypeStruct((count, own, links), BF16),
            jax.ShapeDtypeStruct((size, size), F32),
            jax.ShapeDtypeStruct((size, size), F32),
            jax.ShapeDtypeStruct((size, 128), F32),
            jax.ShapeDtypeStruct((8, 128), F32),
        ),
        in_specs=[vmem] * 3,
        out_specs=(vmem,) * 5,
        scratch_shapes=[
            pltpu.VMEM((count, obs, 128), jnp.int32),
            pltpu.VMEM((count, 8, 128), F32),
            pltpu.VMEM((own, total), BF16),
            pltpu.VMEM((members, regions, own, total), BF16),
            pltpu.VMEM((8, total), F32),
            pltpu.VMEM((size, total), BF16),
            pltpu.VMEM((size, total), BF16),
            pltpu.VMEM((size, size), BF16),
            pltpu.VMEM((size, size), BF16),
            pltpu.VMEM((size, 2 * size), F32),
            pltpu.VMEM((size, 2 * size), BF16),
            pltpu.VMEM((size, 2 * size), BF16),
        ] + [sems] * 6 + [member_sems] * 2 + [region_sems] * 2 + [pltpu.SemaphoreType.DMA((4,))],
        compiler_params=pltpu.CompilerParams(
            collective_id=0, has_side_effects=True, vmem_limit_bytes=min(56, 20 + total // 64) * MIB),
    )(ensemble, offsets, aux)
    mixed = pl.pallas_call(
        mix_kernel,
        out_shape=jax.ShapeDtypeStruct((size, links), BF16),
        in_specs=[vmem] * 4 + [pl.BlockSpec(memory_space=pl.ANY)],
        out_specs=vmem,
        scratch_shapes=[
            pltpu.VMEM((size, size), F32),
            pltpu.VMEM((size, size), BF16),
            pltpu.VMEM((size, size), BF16),
            pltpu.VMEM((size, 2 * size), F32),
            pltpu.VMEM((size, 2 * size), F32),
            pltpu.SemaphoreType.DMA,
        ],
        compiler_params=pltpu.CompilerParams(vmem_limit_bytes=24 * MIB),
    )(column, scalars, inverse, x.reshape(size, links), system)
    return pl.pallas_call(
        functools.partial(scatter_kernel, members, regions),
        out_shape=jax.ShapeDtypeStruct(ensemble.shape, BF16),
        in_specs=[vmem],
        out_specs=vmem,
        scratch_shapes=[sems, sems, pltpu.SemaphoreType.DMA],
        compiler_params=pltpu.CompilerParams(
            collective_id=1, has_side_effects=True, vmem_limit_bytes=12 * MIB),
    )(mixed.reshape(count, own, links))


def solution(mesh):
    return jax.shard_map(
        local,
        mesh=mesh,
        in_specs=(
            P(("member", "region"), None),
            P("region", "member", None),
            P("region", "member", None),
            P("region", "member", None),
        ),
        out_specs=P(("member", "region"), None),
        check_vma=False,
    )
```

```python
import functools

import jax
import jax.numpy as jnp
from jax import lax
from jax.experimental import pallas as pl
from jax.experimental.pallas import tpu as pltpu
from jax.sharding import PartitionSpec as P

MESH = pl.DeviceIdType.MESH
F32 = jnp.float32
BF16 = jnp.bfloat16
MIB = 1024 * 1024


def peers(members, regions):
    count = members * regions
    own_member, own_region = lax.axis_index("member"), lax.axis_index("region")
    me = own_member * regions + own_region

    def peer(step):
        other = (me + step) % count
        return other, other // regions, other % regions

    return count, me, own_region * members + own_member, peer


def entry_barrier(count, peer):
    barrier = pltpu.get_barrier_semaphore()

    def greet(step, carry):
        _, m, g = peer(step)
        pl.semaphore_signal(barrier, inc=1, device_id=(m, g), device_id_type=MESH)
        return carry

    lax.fori_loop(1, count, greet, 0)
    pl.semaphore_wait(barrier, count - 1)


def halves(value):
    high = value.astype(BF16)
    return high, (value - high.astype(F32)).astype(BF16)


def eye(size, start, columns):
    rows = lax.broadcasted_iota(jnp.int32, (size, columns), 0)
    return (rows == lax.broadcasted_iota(jnp.int32, (size, columns), 1) + start).astype(F32)


def each(total, width, body):
    def step(chunk, carry):
        body(pl.ds(pl.multiple_of(chunk * width, width), width), chunk * width)
        return carry

    lax.fori_loop(0, total // width, step, 0)


dot = functools.partial(jnp.dot, preferred_element_type=F32)
exact = functools.partial(jnp.dot, preferred_element_type=F32, precision=lax.Precision.HIGHEST)


def dot_nt(left, right):
    return lax.dot_general(left, right, (((1,), (1,)), ((), ())), preferred_element_type=F32)


def spectrum_bound(squared, plain):
    norm = jnp.max(jnp.sum(jnp.abs(squared), axis=1, keepdims=True), axis=0, keepdims=True)
    other = jnp.max(jnp.sum(jnp.abs(plain), axis=1, keepdims=True), axis=0, keepdims=True)
    return jnp.minimum(jnp.sqrt(norm) * 1.01, other * 1.0001)


def opening(size, top, a_f, squared, w_f):
    start = 2.0 / (1.0 + top)
    ratio = (top - 1.0) / (top + 1.0)
    scale = 2.0 / (2.0 - ratio * ratio)
    w_f[:, :size] = scale * (2.0 * start * a_f[...] - start * start * squared)
    w_f[:, size:] = scale * start * (2.0 * eye(size, 0, size) - start * a_f[...])
    return ratio * ratio / (2.0 - ratio * ratio)


def gather_kernel(members, regions, source, off, aux, x_out, a_f, inv, col, scal, ens, off_all, aux_all, own_picks, picks,
                  rows, s_h, s_l, a_h, a_l, w_f, w_h, w_l,
                  off_send, off_recv, aux_send, aux_recv, x_send, x_recv, one_send, one_recv, two_send, two_recv,
                  local_sem):
    count, me, my_block, peer = peers(members, regions)
    my_m, my_g = lax.axis_index("member"), lax.axis_index("region")
    links = x_out.shape[2]
    obs = off.shape[0]
    total = own_picks.shape[1]
    size = a_f.shape[0]
    width = min(256, size)
    group = 128 // obs

    own_off = pltpu.make_async_copy(off, off_all.at[my_block], local_sem.at[0])
    own_aux = pltpu.make_async_copy(aux, aux_all.at[my_block], local_sem.at[1])
    own_x = pltpu.make_async_copy(
        ens.at[:, pl.ds(pl.multiple_of(my_block * links, links), links)], x_out.at[me], local_sem.at[2])
    fetch = pltpu.make_async_copy(source, ens, local_sem.at[4])
    fetch.start()
    own_off.start()
    own_aux.start()
    entry_barrier(count, peer)

    def off_copy(step, block_at):
        _, m, g = peer(step)
        return pltpu.make_async_remote_copy(
            off, off_all.at[block_at], off_send.at[step], off_recv.at[block_at], (m, g), MESH)

    def aux_copy(step, block_at):
        _, m, g = peer(step)
        return pltpu.make_async_remote_copy(
            aux, aux_all.at[block_at], aux_send.at[step], aux_recv.at[block_at], (m, g), MESH)

    def x_copy(m, g, row_at):
        block = g * members + m
        return pltpu.make_async_remote_copy(
            ens.at[:, pl.ds(pl.multiple_of(block * links, links), links)],
            x_out.at[row_at], x_send.at[m * regions + g], x_recv.at[row_at], (m, g), MESH)

    def one_copy(m, m_at):
        return pltpu.make_async_remote_copy(
            own_picks, picks.at[m_at, my_g], one_send.at[m], one_recv.at[m_at], (m, my_g), MESH)

    def two_copy(g, g_at):
        return pltpu.make_async_remote_copy(
            picks.at[:, my_g], picks.at[:, g_at], two_send.at[g], two_recv.at[g_at], (my_m, g), MESH)

    def loop(low, high, body):
        def step(at, carry):
            body(at)
            return carry

        lax.fori_loop(low, high, step, 0)

    def next_m(step):
        return (my_m + step) % members

    def next_g(step):
        return (my_g + step) % regions

    loop(1, count, lambda step: off_copy(step, my_block).start())
    loop(1, count, lambda step: aux_copy(step, my_block).start())
    own_off.wait()

    def wait_off(step):
        _, m, g = peer(step)
        off_copy(step, g * members + m).wait_recv()

    loop(1, count, wait_off)
    fetch.wait()
    own_x.start()

    def pick(chunk):
        parts = []
        for at in range(group):
            block = chunk * group + at
            column = off_all[block][:, :1]
            hot = (lax.broadcasted_iota(jnp.int32, (obs, links), 1) == column).astype(F32).astype(BF16)
            values = ens[:, pl.ds(pl.multiple_of(block * links, links), links)]
            parts.append(dot_nt(values, hot))
        own_picks[:, pl.ds(pl.multiple_of(chunk * 128, 128), 128)] = jnp.concatenate(parts, axis=1).astype(BF16)

    loop(0, count // group, pick)
    own_pick = pltpu.make_async_copy(own_picks, picks.at[my_m, my_g], local_sem.at[3])
    own_pick.start()
    loop(1, members, lambda step: one_copy(next_m(step), my_m).start())
    loop(1, members, lambda step: x_copy(next_m(step), my_g, me).start())
    own_pick.wait()
    loop(1, members, lambda step: one_copy(next_m(step), next_m(step)).wait_recv())
    loop(1, regions, lambda step: two_copy(next_g(step), my_g).start())

    def send_rest(step):
        x_copy((my_m + step // (regions - 1)) % members, next_g(1 + step % (regions - 1)), me).start()

    loop(0, members * (regions - 1), send_rest)
    own_aux.wait()

    def wait_aux(step):
        _, m, g = peer(step)
        aux_copy(step, g * members + m).wait_recv()

    loop(1, count, wait_aux)
    lane = lax.broadcasted_iota(jnp.int32, (8, 128), 1) // obs

    def spread_aux(chunk):
        value = jnp.zeros((8, 128), F32)
        for at in range(group):
            value = jnp.where(lane == at, aux_all[chunk * group + at], value)
        rows[:, pl.ds(pl.multiple_of(chunk * 128, 128), 128)] = value

    loop(0, count // group, spread_aux)
    loop(1, regions, lambda step: two_copy(next_g(step), next_g(step)).wait_recv())

    values, variance = rows[0:1, :], rows[1:2, :]
    picked = picks[...].astype(F32).reshape(size, total)
    center = jnp.sum(picked, axis=0, keepdims=True) / size
    anomaly = picked - center
    innovation = values - center
    spread = jnp.sum(anomaly * anomaly, axis=0, keepdims=True) / (size - 1.0) + variance
    lift = jnp.sum(innovation * innovation, axis=1, keepdims=True) / jnp.sum(spread, axis=1, keepdims=True)
    weight = 1.0 / ((size - 1.0) * variance)
    column = jnp.sum(anomaly * (lift * weight * innovation), axis=1, keepdims=True)
    col[...] = jnp.broadcast_to(column, col.shape)
    s_h[...], s_l[...] = halves(anomaly * jnp.sqrt(lift * weight))

    def products(cols, start):
        a_f[:, cols] = eye(size, start, width) + (
            dot_nt(s_h[...], s_h[cols, :]) + dot_nt(s_l[...], s_h[cols, :]) + dot_nt(s_h[...], s_l[cols, :])
        )

    each(size, width, products)
    a_h[...], a_l[...] = halves(a_f[...])

    def square(cols, start):
        inv[:, cols] = (
            dot(a_h[...], a_h[:, cols]) + dot(a_l[...], a_h[:, cols]) + dot(a_h[...], a_l[:, cols])
        )

    each(size, width, square)
    top = spectrum_bound(inv[...], a_f[...])
    scal[...] = jnp.where(lax.broadcasted_iota(jnp.int32, scal.shape, 0) == 0, lift, top)
    bound = opening(size, top, a_f, inv[...], w_f)

    def full_step(count, bound):
        scale = 2.0 / (2.0 - bound * bound)
        w_h[...], w_l[...] = halves(w_f[...])

        def body(cols, start):
            w_f[:, cols] = scale * (2.0 * w_f[:, cols] - (
                dot(w_h[:, :size], w_h[:, cols]) + dot(w_l[:, :size], w_h[:, cols]) + dot(w_h[:, :size], w_l[:, cols])
            ))

        each(2 * size, width, body)
        return bound * bound / (2.0 - bound * bound)

    bound = lax.fori_loop(0, 2, full_step, bound)
    third = 2.0 / (2.0 - bound * bound)
    w_h[...] = w_f[...].astype(BF16)

    def third_step(cols, start):
        w_f[:, cols] = third * (2.0 * w_f[:, cols] - dot(w_h[:, :size], w_h[:, cols]))

    each(2 * size, width, third_step)
    bound = bound * bound / (2.0 - bound * bound)
    scale = 2.0 / (2.0 - bound * bound)
    w_h[...] = w_f[...].astype(BF16)

    def last_step(cols, start):
        right = pl.ds(pl.multiple_of(size + start, width), width)
        w_f[:, right] = scale * (2.0 * w_f[:, right] - dot(w_h[:, :size], w_h[:, right]))

    each(size, width, last_step)
    w_h[:, size:], w_l[:, size:] = halves(w_f[:, size:])

    def correct(cols, start):
        right = pl.ds(pl.multiple_of(size + start, width), width)
        rest = eye(size, start, width) - (
            dot(a_h[...], w_h[:, right]) + dot(a_l[...], w_h[:, right]) + dot(a_h[...], w_l[:, right])
        )
        inv[:, cols] = w_f[:, right] + dot(w_h[:, size:], rest.astype(BF16))

    each(size, width, correct)

    def finish_all(step):
        off_copy(step, my_block).wait_send()
        aux_copy(step, my_block).wait_send()
        other, m, g = peer(step)
        x_copy(m, g, other).wait()

    loop(1, count, finish_all)
    loop(1, members, lambda step: one_copy(next_m(step), my_m).wait_send())
    loop(1, regions, lambda step: two_copy(next_g(step), my_g).wait_send())
    own_x.wait()


def scatter_kernel(members, regions, x, out, send, recv, local_sem):
    count, me, my_block, peer = peers(members, regions)
    links = x.shape[2]

    def columns(block):
        return out.at[:, pl.ds(pl.multiple_of(block * links, links), links)]

    own = pltpu.make_async_copy(x.at[me], columns(my_block), local_sem)
    own.start()
    entry_barrier(count, peer)

    def copy(step, block_at):
        other, m, g = peer(step)
        return pltpu.make_async_remote_copy(
            x.at[other], columns(block_at), send.at[step], recv.at[block_at], (m, g), MESH)

    def start(step, carry):
        copy(step, my_block).start()
        return carry

    def finish(step, carry):
        _, m, g = peer(step)
        copy(step, g * members + m).wait()
        return carry

    lax.fori_loop(1, count, start, 0)
    lax.fori_loop(1, count, finish, 0)
    own.wait()


def mix_kernel(col, scal, inv, x, a_any, out, a_f, m_h, m_l, w_f, z_f, sem):
    size = inv.shape[0]
    width = min(256, size)
    lift = scal[0:1, 0:1]
    inflation = jnp.sqrt(lift)
    column = col[:, :1]

    def finish(inverse):
        gain = jnp.sum(inverse * column, axis=0, keepdims=True)
        m_h[...], m_l[...] = halves(
            0.5 * inflation * (eye(size, 0, size) + inverse) + (gain + (1.0 - inflation) / size))

    gentle = jnp.max(scal[1:2, :]) < 150.0

    @pl.when(gentle)
    def _():
        finish(inv[...])

    @pl.when(jnp.logical_not(gentle))
    def _():
        fetch = pltpu.make_async_copy(a_any, a_f, sem)
        fetch.start()
        fetch.wait()

        def square_exact(cols, start):
            z_f[:, cols] = exact(a_f[...], a_f[:, cols])

        each(size, width, square_exact)
        top = jnp.max(spectrum_bound(z_f[:, :size], a_f[...]))
        bound = opening(size, top, a_f, z_f[:, :size], w_f)

        def going(state):
            return jnp.logical_and(state[0] > 0.01, state[1] < 40)

        def step(state):
            bound, count = state
            scale = 2.0 / (2.0 - bound * bound)

            def body(cols, start):
                z_f[:, cols] = scale * (2.0 * w_f[:, cols] - exact(w_f[:, :size], w_f[:, cols]))

            each(2 * size, width, body)
            w_f[...] = z_f[...]
            return bound * bound / (2.0 - bound * bound), count + 1

        lax.while_loop(going, step, (bound, 0))

        def again(count, carry):
            def residual(cols, start):
                right = pl.ds(pl.multiple_of(size + start, width), width)
                w_f[:, cols] = eye(size, start, width) - exact(a_f[...], w_f[:, right])

            def correct(cols, start):
                right = pl.ds(pl.multiple_of(size + start, width), width)
                z_f[:, cols] = w_f[:, right] + exact(w_f[:, size:], w_f[:, cols])

            each(size, width, residual)
            each(size, width, correct)
            w_f[:, size:] = z_f[:, :size]
            return carry

        lax.fori_loop(0, 2, again, 0)
        finish(z_f[:, :size])

    def apply(cols, start):
        out[:, cols] = (dot(m_h[...], x[:, cols]) + dot(m_l[...], x[:, cols])).astype(BF16)

    each(x.shape[1], width, apply)


def local(ensemble, obs_offset, observed, obs_var):
    members = lax.axis_size("member")
    regions = lax.axis_size("region")
    count = members * regions
    own = ensemble.shape[0]
    size = own * count
    links = ensemble.shape[1] // count
    obs = obs_offset.shape[2]
    total = count * obs
    offsets = jnp.broadcast_to(obs_offset.reshape(obs, 1), (obs, 128))
    aux = jnp.tile(jnp.concatenate([observed.reshape(1, obs), obs_var.reshape(1, obs)], axis=0), (4, 128 // obs))
    vmem = pl.BlockSpec(memory_space=pltpu.VMEM)
    sems = pltpu.SemaphoreType.DMA((count,))
    member_sems = pltpu.SemaphoreType.DMA((members,))
    region_sems = pltpu.SemaphoreType.DMA((regions,))
    x, system, inverse, column, scalars = pl.pallas_call(
        functools.partial(gather_kernel, members, regions),
        out_shape=(
            jax.ShapeDtypeStruct((count, own, links), BF16),
            jax.ShapeDtypeStruct((size, size), F32),
            jax.ShapeDtypeStruct((size, size), F32),
            jax.ShapeDtypeStruct((size, 128), F32),
            jax.ShapeDtypeStruct((8, 128), F32),
        ),
        in_specs=[pl.BlockSpec(memory_space=pltpu.HBM), vmem, vmem],
        out_specs=(vmem,) * 5,
        scratch_shapes=[
            pltpu.VMEM(ensemble.shape, BF16),
            pltpu.VMEM((count, obs, 128), jnp.int32),
            pltpu.VMEM((count, 8, 128), F32),
            pltpu.VMEM((own, total), BF16),
            pltpu.VMEM((members, regions, own, total), BF16),
            pltpu.VMEM((8, total), F32),
            pltpu.VMEM((size, total), BF16),
            pltpu.VMEM((size, total), BF16),
            pltpu.VMEM((size, size), BF16),
            pltpu.VMEM((size, size), BF16),
            pltpu.VMEM((size, 2 * size), F32),
            pltpu.VMEM((size, 2 * size), BF16),
            pltpu.VMEM((size, 2 * size), BF16),
        ] + [sems] * 6 + [member_sems] * 2 + [region_sems] * 2 + [pltpu.SemaphoreType.DMA((5,))],
        compiler_params=pltpu.CompilerParams(
            collective_id=0, has_side_effects=True, vmem_limit_bytes=min(56, 20 + total // 64) * MIB),
    )(ensemble, offsets, aux)
    mixed = pl.pallas_call(
        mix_kernel,
        out_shape=jax.ShapeDtypeStruct((size, links), BF16),
        in_specs=[vmem] * 4 + [pl.BlockSpec(memory_space=pl.ANY)],
        out_specs=vmem,
        scratch_shapes=[
            pltpu.VMEM((size, size), F32),
            pltpu.VMEM((size, size), BF16),
            pltpu.VMEM((size, size), BF16),
            pltpu.VMEM((size, 2 * size), F32),
            pltpu.VMEM((size, 2 * size), F32),
            pltpu.SemaphoreType.DMA,
        ],
        compiler_params=pltpu.CompilerParams(vmem_limit_bytes=24 * MIB),
    )(column, scalars, inverse, x.reshape(size, links), system)
    return pl.pallas_call(
        functools.partial(scatter_kernel, members, regions),
        out_shape=jax.ShapeDtypeStruct(ensemble.shape, BF16),
        in_specs=[vmem],
        out_specs=vmem,
        scratch_shapes=[sems, sems, pltpu.SemaphoreType.DMA],
        compiler_params=pltpu.CompilerParams(
            collective_id=1, has_side_effects=True, vmem_limit_bytes=12 * MIB),
    )(mixed.reshape(count, own, links))


def solution(mesh):
    return jax.shard_map(
        local,
        mesh=mesh,
        in_specs=(
            P(("member", "region"), None),
            P("region", "member", None),
            P("region", "member", None),
            P("region", "member", None),
        ),
        out_specs=P(("member", "region"), None),
        check_vma=False,
    )
```
